32 devices in a mesh: dp: 4 (over x, y), tp: 8 (over z, core).
Axes of the slice: x: 2, y: 2, z: 4, core: 2. Of those that a mesh axis runs over, the one named last changes fastest.
Arguments:
- x: bfloat16 [16384, 2048], P(('dp', 'tp')), parts along dimension 0
- dy: bfloat16 [16384, 2048], P(('dp', 'tp')), parts along dimension 0
- gain: bfloat16 [2048], replicated
- wq: bfloat16 [2048, 2048], P(None, 'tp')
- wk: bfloat16 [2048, 2048], P(None, 'tp')
- wv: bfloat16 [2048, 2048], P(None, 'tp')
- wo: bfloat16 [2048, 2048], P('tp')
Outputs:
- output 1: bfloat16 [16384, 2048], P(('dp', 'tp')), parts along dimension 0
- output 2: float32 [4, 2048], P('dp'), parts along dimension 0
- output 3: bfloat16 [8192, 2048], P('dp', 'tp'), parts along dimension 0
- output 4: bfloat16 [8192, 2048], P('dp', 'tp'), parts along dimension 0
- output 5: bfloat16 [8192, 2048], P('dp', 'tp'), parts along dimension 0
- output 6: bfloat16 [8192, 2048], P(('dp', 'tp')), parts along dimension 0
There are 4 independent parts. The reference program is written for one: setup_inputs(seed, part) draws one part's arguments, and reference() takes and returns one part's arrays. A program takes and returns all parts, laid end to end along the dimension named above; an argument that names none is the same for every part.
All inputs are finite; a program needn't handle non-finite values.
Results may differ from the reference program's by a relative error of at most 0.018.
Values are sent between devices in bfloat16 or wider.
A program may use at most 2 GiB of HBM per device.

```python
import jax
import jax.numpy as jnp
from jax import lax

ROWS = 4096
D = 2048
HEADS = 16
KV_HEADS = 16
HEAD = 128
THETA = 10000


def setup_inputs(seed: int = 0, part: int = 0) -> dict:
    kx, ky, kn, kq, kk, kv, ko = jax.random.split(jax.random.key(seed), 7)

    def weights(key, rows, columns):
        return jax.random.normal(key, (rows, columns), jnp.float32) * rows**-0.5

    drawn = {
        "x": jax.random.normal(jax.random.fold_in(kx, part), (ROWS, D), jnp.float32),
        "dy": jax.random.normal(jax.random.fold_in(ky, part), (ROWS, D), jnp.float32) * ROWS**-0.5,
        "gain": 1 + 0.1 * jax.random.normal(kn, (D,), jnp.float32),
        "wq": 2 * weights(kq, D, HEADS * HEAD),
        "wk": 2 * weights(kk, D, KV_HEADS * HEAD),
        "wv": 4 * weights(kv, D, KV_HEADS * HEAD),
        "wo": weights(ko, HEADS * HEAD, D),
    }
    return {k: v.astype(jnp.bfloat16) for k, v in drawn.items()}


def normed(x, gain):
    wide = x.astype(jnp.float32)
    scale = lax.rsqrt(jnp.mean(wide * wide, -1, keepdims=True) + 1e-6)
    return (wide * scale * gain.astype(jnp.float32)).astype(jnp.bfloat16)


def turned(t, place, theta):
    half = t.shape[-1] // 2
    angle = place.astype(jnp.float32)[:, None] * theta ** (-jnp.arange(half, dtype=jnp.float32) / half)
    cos, sin = jnp.cos(angle)[:, None], jnp.sin(angle)[:, None]
    a, b = t[..., :half].astype(jnp.float32), t[..., half:].astype(jnp.float32)
    return jnp.concatenate([a * cos - b * sin, b * cos + a * sin], -1).astype(jnp.bfloat16)


def matmul(a, w):
    return jnp.dot(a, w, preferred_element_type=jnp.float32).astype(jnp.bfloat16)


def einsum(form, a, b):
    return jnp.einsum(form, a.astype(jnp.float32), b.astype(jnp.float32))


def attention(q, k, v):
    scores = einsum("tgsd,ugd->gstu", q, k) * q.shape[-1] ** -0.5
    token = jnp.arange(q.shape[0])
    scores = jnp.where(token[:, None] >= token, scores, -jnp.inf)
    weights = jax.nn.softmax(scores, -1).astype(jnp.bfloat16)
    return einsum("gstu,ugd->tgsd", weights, v).astype(jnp.bfloat16)


def forward(x, gain, wq, wk, wv, wo):
    rows = x.shape[0]
    a, place = normed(x, gain), jnp.arange(rows)
    k = turned(matmul(a, wk).reshape(rows, -1, HEAD), place, THETA)
    q = turned(matmul(a, wq).reshape(rows, -1, HEAD), place, THETA).reshape(rows, k.shape[1], -1, HEAD)
    v = matmul(a, wv).reshape(rows, -1, HEAD)
    seen = attention(q, k, v).reshape(rows, -1)
    return (x.astype(jnp.float32) + jnp.dot(seen, wo, preferred_element_type=jnp.float32)).astype(jnp.bfloat16)


def reference(x, dy, gain, wq, wk, wv, wo):
    _, back = jax.vjp(forward, x, gain.astype(jnp.float32), wq, wk, wv, wo)
    by_x, by_gain, *by_weights = back(dy)
    return (by_x, by_gain[None], *by_weights)
```

```python
import jax
import jax.numpy as jnp
from jax import lax
from jax.experimental import pallas as pl
from jax.experimental.pallas import tpu as pltpu
from jax.sharding import PartitionSpec as P

HEAD = 128
THETA = 10000
NEG = -1e30
HIDDEN = 2 * NEG
LOG2E = 1.4426950408889634
MESH = pl.DeviceIdType.MESH
F32, BF16 = jnp.float32, jnp.bfloat16

CHIPS = 4
MINE = 512
PART = 256
WIDE = 2048
CHUNK = 2 * MINE
ROWS = CHIPS * CHUNK
SCALE = HEAD**-0.5
E2 = SCALE * LOG2E
BK = 512


def _dot(a, b, ca, cb):
    return lax.dot_general(a, b, (((ca,), (cb,)), ((), ())), preferred_element_type=F32)


def _pick(i, values):
    out = jnp.int32(values[-1])
    for n in range(len(values) - 2, -1, -1):
        out = jnp.where(i == n, jnp.int32(values[n]), out)
    return out


def _kernel(a_ref, dy_ref, cosf, sinf, cosc, sinc, wq, wk, wv, wo,
            xf, dyf, da_ref, dwq, dwk, dwv, dwo, rin, lin, sin,
            q_s, k_s, v_s, out_s, do_s, lse_s, del_s, top_s, mix_s, dq_s, dk_s, dv_s, g_s, acc, tile, st, so, fin,
            xs, xr, ys, yr, ss, sr, rs, rr, lr, loc, tsem, fsem):
    me = lax.axis_index("tp")
    z, c = lax.div(me, 2), lax.rem(me, 2)
    sib = me + 1 - 2 * c

    def rows(d, p):
        return pl.ds(pl.multiple_of(d * MINE + p * PART, PART), PART)

    def push(own, full, sends, recvs, d, p, kind, target, first):
        src = own.at[pl.ds(p * PART, PART), :] if first else full.at[rows(d, p), :]
        pltpu.make_async_remote_copy(src_ref=src, dst_ref=full.at[rows(d, p), :], send_sem=sends.at[kind, d, p],
                                     recv_sem=recvs.at[d, p], device_id={"tp": target}, device_id_type=MESH).start()

    def waiting(full, sends, recvs, d, p, kind):
        return pltpu.make_async_remote_copy(src_ref=full.at[rows(d, p), :], dst_ref=full.at[rows(d, p), :], send_sem=sends.at[kind, d, p],
                                            recv_sem=recvs.at[d, p], device_id={"tp": sib}, device_id_type=MESH)

    X, Y = (a_ref, xf, xs, xr), (dy_ref, dyf, ys, yr)

    def own_right(t):
        for p in range(2):
            push(*t, me, p, 0, me + 2, True)

    def own_left(t):
        for p in range(2):
            push(*t, me, p, 1, me - 2, True)

    def own_side(t):
        for p in range(2):
            push(*t, me, p, 2, sib, True)

    def arrive(t, n):
        d = 2 * n + c
        right = n < z
        more = jnp.where(right, z < CHIPS - 1, z > 0)
        ahead = me + jnp.where(right, 2, -2)
        for p in range(2):
            waiting(*t[1:], d, p, 0).wait_recv()

            @pl.when(more)
            def _():
                push(*t, d, p, 0, ahead, False)

            push(*t, d, p, 2, sib, False)

    barrier = pltpu.get_barrier_semaphore()
    pl.semaphore_signal(barrier, inc=1, device_id={"tp": sib}, device_id_type=MESH)

    @pl.when(z < CHIPS - 1)
    def _():
        pl.semaphore_signal(barrier, inc=1, device_id={"tp": me + 2}, device_id_type=MESH)

    @pl.when(z > 0)
    def _():
        pl.semaphore_signal(barrier, inc=1, device_id={"tp": me - 2}, device_id_type=MESH)

    pl.semaphore_wait(barrier, 1 + jnp.where(z < CHIPS - 1, 1, 0) + jnp.where(z > 0, 1, 0))

    @pl.when(z < CHIPS - 1)
    def _():
        own_right(X)

    @pl.when(z > 0)
    def _():
        own_left(X)

    own_side(X)

    @pl.when(z == 0)
    def _():
        own_right(Y)

    @pl.when(z == CHIPS - 1)
    def _():
        own_left(Y)

    own_side(Y)
    dk_s[...] = jnp.zeros_like(dk_s)
    dv_s[...] = jnp.zeros_like(dv_s)
    acc[...] = jnp.zeros_like(acc)

    def angles(row):
        b = pl.ds(lax.div(row, 256), 1)
        cc, sc = cosc[b, :], sinc[b, :]
        cos = cc * cosf[...] - sc * sinf[...]
        s = sc * cosf[...] + cc * sinf[...]
        lane = lax.broadcasted_iota(jnp.int32, (256, HEAD), 1)
        return cos, jnp.where(lane < HEAD // 2, -s, s)

    def fetch(t, d, slot):
        @pl.when(d == me)
        def _():
            pltpu.make_async_copy(t[0], tile.at[slot], tsem.at[slot]).start()

        @pl.when(d != me)
        def _():
            pltpu.make_async_copy(t[1].at[pl.ds(pl.multiple_of(d * MINE, MINE), MINE), :], tile.at[slot], tsem.at[slot]).start()

    def fetched(t, slot):
        pltpu.make_async_copy(t[0], tile.at[slot], tsem.at[slot]).wait()

    def project(i, _):
        j, h = lax.div(i, 2), lax.rem(i, 2)
        n = jnp.where(j == 0, z, jnp.where(j == 1, _pick(z, [1, 0, 1, 2]), jnp.where(j == 2, _pick(z, [2, 2, 3, 1]), _pick(z, [3, 3, 0, 0]))))
        d = 2 * n + jnp.where(h == 0, c, 1 - c)

        @pl.when((h == 0) & (j > 0))
        def _():
            arrive(X, n)

        @pl.when(h == 1)
        def _():
            for p in range(2):
                waiting(*X[1:], d, p, 0).wait_recv()

        fetch(X, d, 0)
        fetched(X, 0)

        def sub(t, _):
            row = pl.multiple_of(d * MINE + t * 256, 256)
            some = tile[0, pl.ds(pl.multiple_of(t * 256, 256), 256), :]
            cos, sgn = angles(row)
            for w, to, turn in ((wq, q_s, True), (wk, k_s, True), (wv, v_s, False)):
                got = _dot(some, w[...], 1, 0).astype(BF16)
                for head in range(2):
                    one = got[:, head * HEAD : (head + 1) * HEAD]
                    if turn:
                        wide = one.astype(F32)
                        one = (wide * cos + pltpu.roll(wide, HEAD // 2, 1) * sgn).astype(BF16)
                    to[head, pl.ds(row, 256), :] = one

        lax.fori_loop(0, 2, sub, None)

    lax.fori_loop(0, 2 * CHIPS, project, None)

    @pl.when((z == 1) | (z == 2))
    def _():
        own_right(Y)
        arrive(Y, 3)

    @pl.when(z == 2)
    def _():
        own_left(Y)

    seen = lax.broadcasted_iota(jnp.int32, (BK, BK), 1) >= lax.broadcasted_iota(jnp.int32, (BK, BK), 0)
    ones = jnp.ones((8, BK), BF16)
    WHOLE = [(0, 0, False), (0, 1, False), (1, 0, False), (1, 1, False)]
    CUT = [(0, 0, True), (0, 1, False), (1, 0, True), (1, 1, False)]
    LAST = [(0, 1, True), (1, 1, True)]

    def strip(n, s):
        return pl.ds(pl.multiple_of(n * CHUNK + s * BK, BK), BK)

    def cols(s):
        return pl.ds(s * BK, BK)

    def ahead(n, _):
        top_s[...] = jnp.full_like(top_s, NEG)
        mix_s[...] = jnp.zeros_like(mix_s)

        def block(j, pieces):
            here = pl.ds(pl.multiple_of(j * BK, BK), BK)
            scores = [_dot(k_s[i, here, :], q_s[i, strip(n, s), :], 1, 1) for i, s, _ in pieces]
            weights, keeps = [], []
            for (i, s, masked), sc in zip(pieces, scores):
                if masked:
                    sc = jnp.where(seen, sc, HIDDEN)
                old = top_s[i : i + 1, cols(s)]
                top = jnp.maximum(old, sc.max(axis=0, keepdims=True))
                top_s[i : i + 1, cols(s)] = top
                weights.append(jnp.exp2((sc - top) * E2).astype(BF16))
                keeps.append(jnp.exp2((old - top) * E2))
            for (i, s, _), p, keep in zip(pieces, weights, keeps):
                values = jnp.concatenate([v_s[i, here, :].T, ones], axis=0)
                mix_s[i, :, cols(s)] = mix_s[i, :, cols(s)] * keep + _dot(values, p, 1, 0)

        lax.fori_loop(0, 2 * n, lambda j, _: block(j, WHOLE), None)
        block(2 * n, CUT)
        block(2 * n + 1, LAST)
        here = pl.ds(pl.multiple_of(n * CHUNK, CHUNK), CHUNK)
        for i in range(2):
            total = mix_s[i, HEAD : HEAD + 1, :]
            out_s[i, here, :] = (mix_s[i, :HEAD, :] * (1 / total)).T.astype(BF16)
            lse_s[i : i + 1, here] = top_s[i : i + 1, :] * E2 + jnp.log(total) * LOG2E

    lax.fori_loop(0, CHIPS, ahead, None)

    def term(row, store):
        def sub(b, _):
            at = pl.ds(pl.multiple_of(b * 512, 512), 512)
            total = None
            for m, w in enumerate((wq, wk, wv)):
                t = _dot(g_s[pl.ds(row, 256), m * 256 : (m + 1) * 256], w[at, :], 1, 1)
                total = t if total is None else total + t
            store(at, total)

        lax.fori_loop(0, WIDE // 512, sub, None)

    def side_copy(n, p):
        return pltpu.make_async_remote_copy(src_ref=st.at[p], dst_ref=sin.at[n, p], send_sem=ss.at[p], recv_sem=sr.at[n, p],
                                            device_id={"tp": sib}, device_id_type=MESH)

    def line_copy(n, p, right):
        if right:
            return pltpu.make_async_remote_copy(src_ref=so.at[p], dst_ref=rin.at[n, p], send_sem=rs.at[p], recv_sem=rr.at[n, p],
                                                device_id={"tp": me + 2}, device_id_type=MESH)
        return pltpu.make_async_remote_copy(src_ref=so.at[p], dst_ref=lin.at[n, p], send_sem=rs.at[p], recv_sem=lr.at[n, p],
                                            device_id={"tp": me - 2}, device_id_type=MESH)

    def back(k):
        n = CHIPS - 1 - k

        @pl.when((k == 0) & (z == 0))
        def _():
            arrive(Y, 3)

        @pl.when((k == 0) & (z == 1))
        def _():
            arrive(Y, 0)
            arrive(Y, 2)
            own_left(Y)

        @pl.when((k == 0) & (z == 2))
        def _():
            arrive(Y, 1)

        @pl.when((k == 0) & (z == 3))
        def _():
            arrive(Y, 2)

        @pl.when((k == 1) & (z == 0))
        def _():
            arrive(Y, 2)

        @pl.when((k == 1) & (z == 2))
        def _():
            arrive(Y, 0)

        @pl.when((k == 2) & ((z == 0) | (z == 3)))
        def _():
            arrive(Y, 1)

        @pl.when((k == 3) & (z == 3))
        def _():
            arrive(Y, 0)

        for p in range(2):
            waiting(*Y[1:], 2 * n + 1 - c, p, 0).wait_recv()
        for h in range(2):
            fetch(Y, 2 * n + h, h)
        for h in range(2):
            fetched(Y, h)

            def sub(t, _):
                some = tile[h, pl.ds(pl.multiple_of(t * 256, 256), 256), :]
                got = _dot(some, wo[...], 1, 1).astype(BF16)
                at = pl.ds(pl.multiple_of(h * MINE + t * 256, 256), 256)
                for i in range(2):
                    do_s[i, at, :] = got[:, i * HEAD : (i + 1) * HEAD]

            lax.fori_loop(0, 2, sub, None)
            mixed = pl.ds(pl.multiple_of(n * CHUNK + h * MINE, MINE), MINE)
            for i in range(2):
                turned = out_s[i, mixed, :].T

                def wide(b, _):
                    at = pl.ds(pl.multiple_of(b * 512, 512), 512)
                    acc[i * HEAD : (i + 1) * HEAD, at] += _dot(turned, tile[h, :, at], 1, 0)

                lax.fori_loop(0, WIDE // 512, wide, None)
        here = pl.ds(pl.multiple_of(n * CHUNK, CHUNK), CHUNK)
        for i in range(2):
            del_s[i : i + 1, :] = (do_s[i].astype(F32) * out_s[i, here, :].astype(F32)).T.sum(axis=0, keepdims=True)
        dq_s[...] = jnp.zeros_like(dq_s)

        def block(j, pieces):
            keys = pl.ds(pl.multiple_of(j * BK, BK), BK)
            qs = [q_s[i, strip(n, s), :] for i, s, _ in pieces]
            dos = [do_s[i, cols(s), :] for i, s, _ in pieces]
            scores = [_dot(k_s[i, keys, :], x, 1, 1) for (i, _, _), x in zip(pieces, qs)]
            dps = [_dot(v_s[i, keys, :], x, 1, 1) for (i, _, _), x in zip(pieces, dos)]
            for m, (i, s, masked) in enumerate(pieces):
                p = jnp.exp2(scores[m] * E2 - lse_s[i : i + 1, strip(n, s)])
                if masked:
                    p = jnp.where(seen, p, 0.0)
                ds = (p * (dps[m] - del_s[i : i + 1, cols(s)])).astype(BF16)
                dv_s[i, keys, :] += _dot(p.astype(BF16), dos[m], 1, 0)
                dk_s[i, keys, :] += _dot(ds, qs[m], 1, 0)
                dq_s[i, :, cols(s)] += _dot(k_s[i, keys, :].T, ds, 1, 0)

        lax.fori_loop(0, 2 * n, lambda j, _: block(j, WHOLE), None)
        block(2 * n, CUT)
        block(2 * n + 1, LAST)

        for t in range(CHUNK // 256):
            row = pl.multiple_of(n * CHUNK + t * 256, 256)
            cos, sgn = angles(row)
            for i in range(2):
                dq = (dq_s[i, :, t * 256 : (t + 1) * 256] * SCALE).T
                dk = dk_s[i, pl.ds(row, 256), :] * SCALE
                for m, one in ((0, dq), (1, dk)):
                    g_s[pl.ds(row, 256), m * 256 + i * HEAD : m * 256 + (i + 1) * HEAD] = (
                        one * cos - pltpu.roll(one, HEAD // 2, 1) * sgn).astype(BF16)
                g_s[pl.ds(row, 256), 512 + i * HEAD : 512 + (i + 1) * HEAD] = dv_s[i, pl.ds(row, 256), :].astype(BF16)

        for p in range(2):
            @pl.when(k > 0)
            def _():
                side_copy(n, p).wait_send()

            def store(at, value):
                st[p, :, at] = value.astype(BF16)

            term(pl.multiple_of((2 * n + 1 - c) * MINE + p * PART, PART), store)
            side_copy(n, p).start()

    def relay(n, again):
        from_left = (z <= n) & (z > 0)
        from_right = (z >= n) & (z < CHIPS - 1)
        ld = [tile.at[0, pl.ds(0, PART), :], tile.at[0, pl.ds(PART, PART), :], tile.at[1, pl.ds(0, PART), :]]
        for p in range(2):
            side_copy(n, p).wait_recv()
            pltpu.make_async_copy(sin.at[n, p], ld[0], loc.at[0]).start()

            @pl.when(from_left)
            def _():
                line_copy(n, p, True).wait_recv()
                pltpu.make_async_copy(rin.at[n, p], ld[1], loc.at[1]).start()

            @pl.when(from_right)
            def _():
                line_copy(n, p, False).wait_recv()
                pltpu.make_async_copy(lin.at[n, p], ld[2], loc.at[2]).start()

            def store(at, value):
                fin[:, at] = value

            @pl.when((z == n) & (p == 1))
            def _():
                pltpu.make_async_copy(fin, da_ref.at[pl.ds(0, PART), :], fsem).wait()

            term(pl.multiple_of((2 * n + c) * MINE + p * PART, PART), store)
            pltpu.make_async_copy(sin.at[n, p], ld[0], loc.at[0]).wait()
            fin[...] += ld[0][...].astype(F32)

            @pl.when(from_left)
            def _():
                pltpu.make_async_copy(rin.at[n, p], ld[1], loc.at[1]).wait()
                fin[...] += ld[1][...].astype(F32)

            @pl.when(from_right)
            def _():
                pltpu.make_async_copy(lin.at[n, p], ld[2], loc.at[2]).wait()
                fin[...] += ld[2][...].astype(F32)

            @pl.when(z == n)
            def _():
                pltpu.make_async_copy(fin, da_ref.at[pl.ds(p * PART, PART), :], fsem).start()

            @pl.when(z != n)
            def _():
                @pl.when(again)
                def _():
                    line_copy(n, p, True).wait_send()

                so[p] = fin[...].astype(BF16)

                @pl.when(z < n)
                def _():
                    line_copy(n, p, True).start()

                @pl.when(z > n)
                def _():
                    line_copy(n, p, False).start()

    def weight(m, to):
        fetch(X, 0, 0)
        acc[...] = jnp.zeros_like(acc)

        def step(d, _):
            slot = lax.rem(d, 2)

            @pl.when(d + 1 < 2 * CHIPS)
            def _():
                fetch(X, d + 1, 1 - slot)

            fetched(X, slot)
            turned = g_s[pl.ds(pl.multiple_of(d * MINE, MINE), MINE), m * 256 : (m + 1) * 256].T

            def wide(b, _):
                at = pl.ds(pl.multiple_of(b * 512, 512), 512)
                acc[:, at] += _dot(turned, tile[slot, :, at], 1, 0)

            lax.fori_loop(0, WIDE // 512, wide, None)

        lax.fori_loop(0, 2 * CHIPS, step, None)

        def turn(b, _):
            at = pl.ds(pl.multiple_of(b * 256, 256), 256)
            to[at, :] = acc[:, at].T.astype(BF16)

        lax.fori_loop(0, WIDE // 256, turn, None)

    SLOTS = [[3, -1, -1, -1], [2, 3, -1, 2], [1, 2, 3, -1], [-1, -1, -1, 0], [-1, 0, 0, 1], [-1, -1, 1, -1], [0, 1, 2, 3]]
    AGAIN = [[0, 0, 0, 0], [1, 0, 0, 0], [1, 1, 0, 0], [0, 0, 0, 1], [0, 1, 1, 1], [0, 0, 1, 0], [0, 0, 0, 0]]

    def slot(k, _):
        @pl.when(k < CHIPS)
        def _():
            back(k)

        @pl.when(k == CHIPS - 1)
        def _():
            dwo[...] = acc[...].astype(BF16)

        n, again = jnp.int32(-1), jnp.int32(0)
        for i in range(len(SLOTS)):
            n = jnp.where(k == i, _pick(z, SLOTS[i]), n)
            again = jnp.where(k == i, _pick(z, AGAIN[i]), again)

        @pl.when(n >= 0)
        def _():
            relay(n, again > 0)

        @pl.when(k == 3)
        def _():
            weight(0, dwq)

        @pl.when(k == 4)
        def _():
            weight(1, dwk)

        @pl.when(k == 5)
        def _():
            weight(2, dwv)


    lax.fori_loop(0, len(SLOTS), slot, None)

    pltpu.make_async_copy(fin, da_ref.at[pl.ds(PART, PART), :], fsem).wait()
    for p in range(2):
        side_copy(0, p).wait_send()
        line_copy(0, p, True).wait_send()
        for t in (X, Y):
            @pl.when(z < CHIPS - 1)
            def _():
                waiting(*t[1:], me, p, 0).wait_send()

            @pl.when(z > 0)
            def _():
                waiting(*t[1:], me, p, 1).wait_send()

            for n in range(CHIPS):
                waiting(*t[1:], 2 * n + c, p, 2).wait_send()

                @pl.when(((n < z) & (z < CHIPS - 1)) | ((n > z) & (z > 0)))
                def _():
                    waiting(*t[1:], 2 * n + c, p, 0).wait_send()


def heads_work(a, dy, wq, wk, wv, wo):
    half = HEAD // 2
    rate = THETA ** (-jnp.arange(half, dtype=F32) / half)
    rate = jnp.concatenate([rate, rate])
    fine, coarse = jnp.arange(256, dtype=F32)[:, None] * rate, (256 * jnp.arange(ROWS // 256, dtype=F32))[:, None] * rate
    any_, vmem = pl.BlockSpec(memory_space=pl.ANY), pl.BlockSpec(memory_space=pltpu.VMEM)
    S = jax.ShapeDtypeStruct
    DMA = pltpu.SemaphoreType.DMA
    comm = S((CHIPS, 2, PART, WIDE), BF16)
    outs = pl.pallas_call(
        _kernel,
        in_specs=[any_, any_] + [vmem] * 8,
        out_specs=[any_] * 3 + [vmem] * 4 + [any_] * 3,
        out_shape=[S((ROWS, WIDE), BF16), S((ROWS, WIDE), BF16), S((MINE, WIDE), F32),
                   S((WIDE, 256), BF16), S((WIDE, 256), BF16), S((WIDE, 256), BF16), S((256, WIDE), BF16), comm, comm, comm],
        scratch_shapes=[
            pltpu.VMEM((2, ROWS, HEAD), BF16), pltpu.VMEM((2, ROWS, HEAD), BF16), pltpu.VMEM((2, ROWS, HEAD), BF16),
            pltpu.VMEM((2, ROWS, HEAD), BF16), pltpu.VMEM((2, CHUNK, HEAD), BF16),
            pltpu.VMEM((2, ROWS), F32), pltpu.VMEM((2, CHUNK), F32), pltpu.VMEM((2, CHUNK), F32),
            pltpu.VMEM((2, HEAD + 8, CHUNK), F32), pltpu.VMEM((2, HEAD, CHUNK), F32),
            pltpu.VMEM((2, ROWS, HEAD), F32), pltpu.VMEM((2, ROWS, HEAD), F32),
            pltpu.VMEM((ROWS, 768), BF16), pltpu.VMEM((256, WIDE), F32), pltpu.VMEM((2, MINE, WIDE), BF16),
            pltpu.VMEM((2, PART, WIDE), BF16), pltpu.VMEM((2, PART, WIDE), BF16),
            pltpu.VMEM((PART, WIDE), F32),
            DMA((3, 8, 2)), DMA((8, 2)), DMA((3, 8, 2)), DMA((8, 2)),
            DMA((2,)), DMA((CHIPS, 2)), DMA((2,)), DMA((CHIPS, 2)), DMA((CHIPS, 2)), DMA((3,)), DMA((2,)), DMA,
        ],
        compiler_params=pltpu.CompilerParams(collective_id=0, has_side_effects=True, vmem_limit_bytes=67043328 - 2**20),
    )(a, dy, jnp.cos(fine), jnp.sin(fine), jnp.cos(coarse), jnp.sin(coarse), wq, wk, wv, wo)
    return outs[2:7]


def solution(mesh):
    def step(x, dy, gain, wq, wk, wv, wo):
        wide, gain = x.astype(F32), gain.astype(F32)
        scale = lax.rsqrt(jnp.mean(wide * wide, -1, keepdims=True) + 1e-6)
        a = (wide * scale * gain).astype(BF16)
        da, *by_weights = heads_work(a, dy, wq, wk, wv, wo)
        unit = wide * scale
        by_gain = lax.psum((da * unit).sum(0), "tp")
        t = da * gain
        by_x = scale * (t - unit * jnp.mean(t * unit, -1, keepdims=True)) + dy.astype(F32)
        return (by_x.astype(BF16), by_gain[None], *by_weights)

    tokens, columns = P(("dp", "tp"), None), P(None, "tp")
    return jax.shard_map(
        step,
        mesh=mesh,
        in_specs=(tokens, tokens, P(None), columns, columns, columns, P("tp", None)),
        out_specs=(tokens, P("dp", None), P("dp", "tp"), P("dp", "tp"), P("dp", "tp"), P(("dp", "tp"), None)),
        check_vma=False,
    )
```

```python
import jax
import jax.numpy as jnp
import numpy as np
from jax import lax
from jax.experimental import pallas as pl
from jax.experimental.pallas import tpu as pltpu
from jax.sharding import PartitionSpec as P

HEAD = 128
THETA = 10000
NEG = -1e30
HIDDEN = 2 * NEG
LOG2E = 1.4426950408889634
MESH = pl.DeviceIdType.MESH
F32, BF16 = jnp.float32, jnp.bfloat16

CHIPS = 4
MINE = 512
PART = 256
WIDE = 2048
CHUNK = 2 * MINE
ROWS = CHIPS * CHUNK
SCALE = HEAD**-0.5
E2 = SCALE * LOG2E
BK = 512
PAIR = range(2)
CORES = 2 * CHIPS
QUART = PART // 2

STEPS = (
    "F3F2A3B3T3U3F1A2B2T2U2F0A1B1T1U1B0W0W1W2W3W4W5T0U0",
    "R0A0F3F2F1A3B3F0A2L0B2B1B0T3U3W0W1W2W3T2W4W5U2T0U0T1U1",
    "A3L0R0F3B3A1F2B2F1A0B1F0B0W0W1W2W3W4W5T3U3T1T0U0T2U1U2",
    "F3B3A2F2B2T2U2F1A1B1T1F0A0B0T0U0U1W0W1W2W3W4W5T3U3",
)
OPS = "-ARLFBTUW"


def _ds(i, size):
    return pl.ds(i * size if isinstance(i, int) else pl.multiple_of(i * size, size), size)


def _program():
    longest = max(map(len, STEPS)) // 2
    words = []
    for i in range(longest):
        word = 0
        for steps in reversed(STEPS):
            op, arg = steps[2 * i : 2 * i + 2] or "-0"
            word = word * 128 + 8 * OPS.index(op) + int(arg)
        words.append(word)
    return words


def _dot(a, b, ca, cb):
    return lax.dot_general(a, b, (((ca,), (cb,)), ((), ())), preferred_element_type=F32)


def _pick(i, values):
    out = jnp.int32(values[-1])
    for n in range(len(values) - 2, -1, -1):
        out = jnp.where(i == n, jnp.int32(values[n]), out)
    return out


def _kernel(a_ref, x_ref, dy_ref, gain, cosf, sinf, cosc, sinc, wq, wk, wv, wo,
            xf, dyf, by_x, by_gain, dwq, dwk, dwv, dwo, rin, lin, sin,
            q_s, k_s, v_s, out_s, do_s, lse_s, del_s, top_s, mix_s, dq_s, dk_s, dv_s, g_s, acc, tile, st, so, fin, gsum, gall,
            xs, xr, ys, yr, ss, sr, rs, rr, lr, loc, tsem, fsem, gs, gr):
    me = lax.axis_index("tp")
    z, c = lax.div(me, 2), lax.rem(me, 2)
    sib = me + 1 - 2 * c

    def rows(d, p):
        return _ds(2 * d + p, PART)

    def push(own, full, sends, recvs, d, p, kind, target, first):
        src = own.at[_ds(p, PART), :] if first else full.at[rows(d, p), :]
        pltpu.make_async_remote_copy(src_ref=src, dst_ref=full.at[rows(d, p), :], send_sem=sends.at[kind, d, p],
                                     recv_sem=recvs.at[d, p], device_id={"tp": target}, device_id_type=MESH).start()

    def waiting(full, sends, recvs, d, p, kind):
        return pltpu.make_async_remote_copy(src_ref=full.at[rows(d, p), :], dst_ref=full.at[rows(d, p), :], send_sem=sends.at[kind, d, p],
                                            recv_sem=recvs.at[d, p], device_id={"tp": sib}, device_id_type=MESH)

    X, Y = (a_ref, xf, xs, xr), (dy_ref, dyf, ys, yr)

    def own_right(t):
        for p in PAIR:
            push(*t, me, p, 0, me + 2, True)

    def own_left(t):
        for p in PAIR:
            push(*t, me, p, 1, me - 2, True)

    def own_side(t):
        for p in PAIR:
            push(*t, me, p, 2, sib, True)

    def arrive(t, n):
        d = 2 * n + c
        right = n < z
        more = jnp.where(right, z < CHIPS - 1, z > 0)
        ahead = me + jnp.where(right, 2, -2)
        for p in PAIR:
            waiting(*t[1:], d, p, 0).wait_recv()

            @pl.when(more)
            def _():
                push(*t, d, p, 0, ahead, False)

            push(*t, d, p, 2, sib, False)

    barrier = pltpu.get_barrier_semaphore()

    def greet(o, _):
        pl.semaphore_signal(barrier, inc=1, device_id={"tp": lax.rem(me + o, CORES)}, device_id_type=MESH)

    lax.fori_loop(1, CORES, greet, None)
    pl.semaphore_wait(barrier, CORES - 1)

    @pl.when(z < CHIPS - 1)
    def _():
        own_right(X)

    @pl.when(z > 0)
    def _():
        own_left(X)

    own_side(X)

    @pl.when(z == 0)
    def _():
        own_right(Y)

    @pl.when(z == CHIPS - 1)
    def _():
        own_left(Y)

    own_side(Y)
    dk_s[:] = jnp.zeros_like(dk_s)
    dv_s[:] = jnp.zeros_like(dv_s)
    acc[:] = jnp.zeros_like(acc)
    gsum[:] = jnp.zeros_like(gsum)

    def angles(row):
        b = pl.ds(lax.div(row, 256), 1)
        cc, sc = cosc[b, :], sinc[b, :]
        cos = cc * cosf[:] - sc * sinf[:]
        s = sc * cosf[:] + cc * sinf[:]
        lane = lax.broadcasted_iota(jnp.int32, (256, HEAD), 1)
        return cos, jnp.where(lane < HEAD // 2, -s, s)

    def fetch(t, d, slot):
        @pl.when(d == me)
        def _():
            pltpu.make_async_copy(t[0], tile.at[slot], tsem.at[slot]).start()

        @pl.when(d != me)
        def _():
            pltpu.make_async_copy(t[1].at[_ds(d, MINE), :], tile.at[slot], tsem.at[slot]).start()

    def fetched(t, slot):
        pltpu.make_async_copy(t[0], tile.at[slot], tsem.at[slot]).wait()

    def project(i, _):
        j, h = lax.div(i, 2), lax.rem(i, 2)
        n = jnp.where(j == 0, z, jnp.where(j == 1, _pick(z, [1, 0, 1, 2]), jnp.where(j == 2, _pick(z, [2, 2, 3, 1]), _pick(z, [3, 3, 0, 0]))))
        d = 2 * n + jnp.where(h == 0, c, 1 - c)

        @pl.when((h == 0) & (j > 0))
        def _():
            arrive(X, n)

        @pl.when(h == 1)
        def _():
            for p in PAIR:
                waiting(*X[1:], d, p, 0).wait_recv()

        fetch(X, d, 0)
        fetched(X, 0)

        def sub(t, _):
            row = pl.multiple_of(d * MINE + t * 256, 256)
            some = tile[0, _ds(t, 256), :]
            cos, sgn = angles(row)
            for w, to, turn in ((wq, q_s, True), (wk, k_s, True), (wv, v_s, False)):
                got = _dot(some, w[:], 1, 0).astype(BF16)
                for head in PAIR:
                    one = got[:, _ds(head, HEAD)]
                    if turn:
                        wide = one.astype(F32)
                        one = (wide * cos + pltpu.roll(wide, HEAD // 2, 1) * sgn).astype(BF16)
                    to[head, pl.ds(row, 256), :] = one

        lax.fori_loop(0, 2, sub, None)

    lax.fori_loop(0, CORES, project, None)

    seen = lax.broadcasted_iota(jnp.int32, (BK, BK), 1) >= lax.broadcasted_iota(jnp.int32, (BK, BK), 0)
    ones = jnp.ones((8, BK), BF16)
    WHOLE = [(0, 0, False), (0, 1, False), (1, 0, False), (1, 1, False)]
    CUT = [(0, 0, True), (0, 1, False), (1, 0, True), (1, 1, False)]
    LAST = [(0, 1, True), (1, 1, True)]

    def strip(n, s):
        return _ds(2 * n + s, BK)

    def cols(s):
        return _ds(s, BK)

    def ahead(n):
        top_s[:] = jnp.full_like(top_s, NEG)
        mix_s[:] = jnp.zeros_like(mix_s)

        def block(j, pieces):
            here = _ds(j, BK)
            scores = [_dot(k_s[i, here, :], q_s[i, strip(n, s), :], 1, 1) for i, s, _ in pieces]
            weights, keeps = [], []
            for (i, s, masked), sc in zip(pieces, scores):
                if masked:
                    sc = jnp.where(seen, sc, HIDDEN)
                old = top_s[i : i + 1, cols(s)]
                top = jnp.maximum(old, sc.max(axis=0, keepdims=True))
                top_s[i : i + 1, cols(s)] = top
                weights.append(jnp.exp2((sc - top) * E2).astype(BF16))
                keeps.append(jnp.exp2((old - top) * E2))
            for (i, s, _), p, keep in zip(pieces, weights, keeps):
                values = jnp.concatenate([v_s[i, here, :].T, ones], axis=0)
                mix_s[i, :, cols(s)] = mix_s[i, :, cols(s)] * keep + _dot(values, p, 1, 0)

        lax.fori_loop(0, 2 * n, lambda j, _: block(j, WHOLE), None)
        block(2 * n, CUT)
        block(2 * n + 1, LAST)
        here = _ds(n, CHUNK)
        for i in PAIR:
            total = mix_s[i, HEAD : HEAD + 1, :]
            out_s[i, here, :] = (mix_s[i, :HEAD, :] * (1 / total)).T.astype(BF16)
            lse_s[i : i + 1, here] = top_s[i : i + 1, :] * E2 + jnp.log(total) * LOG2E

    def term(row, store):
        def sub(b, _):
            at = _ds(b, 512)
            total = None
            for m, w in enumerate((wq, wk, wv)):
                t = _dot(g_s[pl.ds(row, 256), m * 256 : (m + 1) * 256], w[at, :], 1, 1)
                total = t if total is None else total + t
            store(at, total)

        lax.fori_loop(0, WIDE // 512, sub, None)

    def side_copy(n, p):
        return pltpu.make_async_remote_copy(src_ref=st.at[p], dst_ref=sin.at[n, p], send_sem=ss.at[p], recv_sem=sr.at[n, p],
                                            device_id={"tp": sib}, device_id_type=MESH)

    def line_copy(n, s, right):
        recv, to, ahead = (rr, rin, me + 2) if right else (lr, lin, me - 2)
        return pltpu.make_async_remote_copy(src_ref=so.at[s], dst_ref=to.at[n, s], send_sem=rs.at[s], recv_sem=recv.at[n, s],
                                            device_id={"tp": ahead}, device_id_type=MESH)

    def back(n):
        for p in PAIR:
            waiting(*Y[1:], 2 * n + 1 - c, p, 0).wait_recv()
        for h in PAIR:
            fetch(Y, 2 * n + h, h)
        for h in PAIR:
            fetched(Y, h)

            def sub(t, _):
                some = tile[h, _ds(t, 256), :]
                got = _dot(some, wo[:], 1, 1).astype(BF16)
                at = _ds(2 * h + t, 256)
                for i in PAIR:
                    do_s[i, at, :] = got[:, _ds(i, HEAD)]

            lax.fori_loop(0, 2, sub, None)
            mixed = _ds(2 * n + h, MINE)
            for i in PAIR:
                turned = out_s[i, mixed, :].T

                def wide(b, _):
                    at = _ds(b, 512)
                    acc[_ds(i, HEAD), at] += _dot(turned, tile[h, :, at], 1, 0)

                lax.fori_loop(0, WIDE // 512, wide, None)
        here = _ds(n, CHUNK)
        for i in PAIR:
            del_s[i : i + 1, :] = (do_s[i].astype(F32) * out_s[i, here, :].astype(F32)).T.sum(axis=0, keepdims=True)
        dq_s[:] = jnp.zeros_like(dq_s)

        def block(j, pieces):
            keys = _ds(j, BK)
            qs = [q_s[i, strip(n, s), :] for i, s, _ in pieces]
            dos = [do_s[i, cols(s), :] for i, s, _ in pieces]
            scores = [_dot(k_s[i, keys, :], x, 1, 1) for (i, _, _), x in zip(pieces, qs)]
            dps = [_dot(v_s[i, keys, :], x, 1, 1) for (i, _, _), x in zip(pieces, dos)]
            for m, (i, s, masked) in enumerate(pieces):
                p = jnp.exp2(scores[m] * E2 - lse_s[i : i + 1, strip(n, s)])
                if masked:
                    p = jnp.where(seen, p, 0.0)
                ds = (p * (dps[m] - del_s[i : i + 1, cols(s)])).astype(BF16)
                dv_s[i, keys, :] += _dot(p.astype(BF16), dos[m], 1, 0)
                dk_s[i, keys, :] += _dot(ds, qs[m], 1, 0)
                dq_s[i, :, cols(s)] += _dot(k_s[i, keys, :].T, ds, 1, 0)

        lax.fori_loop(0, 2 * n, lambda j, _: block(j, WHOLE), None)
        block(2 * n, CUT)
        block(2 * n + 1, LAST)

        for t in range(CHUNK // 256):
            row = pl.multiple_of(n * CHUNK + t * 256, 256)
            cos, sgn = angles(row)
            for i in PAIR:
                dq = (dq_s[i, :, t * 256 : (t + 1) * 256] * SCALE).T
                dk = dk_s[i, pl.ds(row, 256), :] * SCALE
                for m, one in ((0, dq), (1, dk)):
                    g_s[pl.ds(row, 256), m * 256 + i * HEAD : m * 256 + (i + 1) * HEAD] = (
                        one * cos - pltpu.roll(one, HEAD // 2, 1) * sgn).astype(BF16)
                g_s[pl.ds(row, 256), 512 + i * HEAD : 512 + (i + 1) * HEAD] = dv_s[i, pl.ds(row, 256), :].astype(BF16)

        for p in PAIR:
            @pl.when(n < CHIPS - 1)
            def _():
                side_copy(n, p).wait_send()

            def store(at, value):
                st[p, :, at] = value.astype(BF16)

            term(pl.multiple_of((2 * n + 1 - c) * MINE + p * PART, PART), store)
            side_copy(n, p).start()

        @pl.when(n == 0)
        def _():
            dwo[:] = acc[:].astype(BF16)

    def relay(n, p):
        from_left = (z <= n) & (z > 0)
        from_right = (z >= n) & (z < CHIPS - 1)
        here = tile.at[0, _ds(0, PART), :], tile.at[0, _ds(2, QUART), :], tile.at[0, _ds(3, QUART), :]
        mine = ((x_ref, tile.at[1, _ds(0, PART), :]), (dy_ref, tile.at[1, _ds(1, PART), :]))

        @pl.when(z == n)
        def _():
            for i, (src, dst) in enumerate(mine):
                pltpu.make_async_copy(src.at[_ds(p, PART), :], dst, tsem.at[i]).start()

        side_copy(n, p).wait_recv()
        pltpu.make_async_copy(sin.at[n, p], here[0], loc.at[0]).start()

        def store(at, value):
            fin[:, at] = value

        term(pl.multiple_of((2 * n + c) * MINE + p * PART, PART), store)
        pltpu.make_async_copy(sin.at[n, p], here[0], loc.at[0]).wait()
        fin[:] += here[0][:].astype(F32)

        @pl.when(z == n)
        def _():
            for i, (src, dst) in enumerate(mine):
                pltpu.make_async_copy(src.at[_ds(p, PART), :], dst, tsem.at[i]).wait()

        def quarter(h, _):
            s = 2 * p + h
            part = _ds(h, QUART)
            for i, (come, arrived, right) in enumerate(((from_left, rin, True), (from_right, lin, False))):
                @pl.when(come)
                def _():
                    line_copy(n, s, right).wait_recv()
                    pltpu.make_async_copy(arrived.at[n, s], here[1 + i], loc.at[1 + i]).start()

            for i, (come, arrived, right) in enumerate(((from_left, rin, True), (from_right, lin, False))):
                @pl.when(come)
                def _():
                    pltpu.make_async_copy(arrived.at[n, s], here[1 + i], loc.at[1 + i]).wait()
                    fin[part, :] += here[1 + i][:].astype(F32)

            @pl.when(n != jnp.where(z == CHIPS - 1, CHIPS - 2, CHIPS - 1))
            def _():
                line_copy(n, s, True).wait_send()

            @pl.when(z != n)
            def _():
                so[s] = fin[part, :].astype(BF16)

            @pl.when(z < n)
            def _():
                line_copy(n, s, True).start()

            @pl.when(z > n)
            def _():
                line_copy(n, s, False).start()

            @pl.when(z == n)
            def _():
                def norm(r, _):
                    da = fin[_ds(h * (QUART // 16) + r, 16), :]
                    wide = tile[1, _ds(h * (QUART // 16) + r, 16), :].astype(F32)
                    straight = tile[1, _ds((2 + h) * (QUART // 16) + r, 16), :].astype(F32)
                    scale = lax.rsqrt(jnp.mean(wide * wide, -1, keepdims=True) + 1e-6)
                    unit = wide * scale
                    gsum[:] += da * unit
                    t = da * gain[:]
                    so[s, _ds(r, 16), :] = (scale * (t - unit * jnp.mean(t * unit, -1, keepdims=True)) + straight).astype(BF16)

                lax.fori_loop(0, QUART // 16, norm, None)
                pltpu.make_async_copy(so.at[s], by_x.at[_ds(s, QUART), :], fsem.at[s]).start()

        lax.fori_loop(0, 2, quarter, None)

    def weight(m, h):
        first = h * CHIPS
        fetch(X, first, 0)

        @pl.when(h == 0)
        def _():
            acc[:] = jnp.zeros_like(acc)

        def step(i, _):
            slot = lax.rem(i, 2)

            @pl.when(i + 1 < CHIPS)
            def _():
                fetch(X, first + i + 1, 1 - slot)

            fetched(X, slot)
            turned = g_s[_ds(first + i, MINE), _ds(m, 256)].T

            def wide(b, _):
                at = _ds(b, 512)
                acc[:, at] += _dot(turned, tile[slot, :, at], 1, 0)

            lax.fori_loop(0, WIDE // 512, wide, None)

        lax.fori_loop(0, CHIPS, step, None)
        for i, to in enumerate((dwq, dwk, dwv)):
            @pl.when((h == 1) & (m == i))
            def _():
                def turn(b, _):
                    to[_ds(b, 256), :] = acc[:, _ds(b, 256)].T.astype(BF16)

                lax.fori_loop(0, WIDE // 256, turn, None)

    def step(i, _):
        word = _pick(i, words)
        code = lax.rem(_pick(z, [lax.div(word, jnp.int32(128**n)) for n in range(CHIPS)]), 128)
        op, arg = lax.div(code, 8), lax.rem(code, 8)

        def on(letter, do):
            pl.when(op == OPS.index(letter))(do)

        on("A", lambda: arrive(Y, arg))
        on("R", lambda: own_right(Y))
        on("L", lambda: own_left(Y))
        on("F", lambda: ahead(arg))
        on("B", lambda: back(arg))

        @pl.when((op == OPS.index("T")) | (op == OPS.index("U")))
        def _():
            relay(arg, op - OPS.index("T"))

        on("W", lambda: weight(lax.div(arg, 2), lax.rem(arg, 2)))

    words = _program()
    lax.fori_loop(0, len(words), step, None)

    def sum_copy(o, d):
        return pltpu.make_async_remote_copy(src_ref=gall.at[d], dst_ref=gall.at[d], send_sem=gs.at[o], recv_sem=gr.at[d],
                                            device_id={"tp": lax.rem(me + o, CORES)}, device_id_type=MESH)

    gall[me] = gsum[:].sum(axis=0, keepdims=True)
    lax.fori_loop(1, CORES, lambda o, _: sum_copy(o, me).start(), None)
    lax.fori_loop(1, CORES, lambda o, _: sum_copy(o, lax.rem(me + o, CORES)).wait_recv(), None)
    total = gall[0]
    for d in range(1, CORES):
        total = total + gall[d]
    by_gain[:] = total
    lax.fori_loop(1, CORES, lambda o, _: sum_copy(o, me).wait_send(), None)

    for s in range(MINE // QUART):
        pltpu.make_async_copy(so.at[s], by_x.at[_ds(s, QUART), :], fsem.at[s]).wait()
    for p in PAIR:
        side_copy(0, p).wait_send()
        for t in (X, Y):
            @pl.when(z < CHIPS - 1)
            def _():
                waiting(*t[1:], me, p, 0).wait_send()

            @pl.when(z > 0)
            def _():
                waiting(*t[1:], me, p, 1).wait_send()

            for n in range(CHIPS):
                waiting(*t[1:], 2 * n + c, p, 2).wait_send()

                @pl.when(((n < z) & (z < CHIPS - 1)) | ((n > z) & (z > 0)))
                def _():
                    waiting(*t[1:], 2 * n + c, p, 0).wait_send()


def heads_work(a, x, dy, gain, wq, wk, wv, wo):
    half = HEAD // 2
    rate = np.tile(float(THETA) ** (-np.arange(half) / half), 2)
    fine, coarse = np.arange(PART)[:, None] * rate, np.arange(0, ROWS, PART)[:, None] * rate
    tables = [jnp.asarray(f(t), F32) for t in (fine, coarse) for f in (np.cos, np.sin)]
    any_, vmem = pl.BlockSpec(memory_space=pl.ANY), pl.BlockSpec(memory_space=pltpu.VMEM)
    S = jax.ShapeDtypeStruct
    DMA, VMEM = pltpu.SemaphoreType.DMA, pltpu.VMEM
    heads, chunk = (2, ROWS, HEAD), (2, CHUNK)
    parts, quarts = (MINE // PART, PART, WIDE), (MINE // QUART, QUART, WIDE)
    full, line = S((ROWS, WIDE), BF16), S((CHIPS, *quarts), BF16)
    columns = S(wq.shape, BF16)
    passed, came = DMA((3, CORES, 2)), DMA((CORES, 2))
    outs = pl.pallas_call(
        _kernel,
        in_specs=[any_] * 3 + [vmem] * 9,
        out_specs=[any_] * 3 + [vmem] * 5 + [any_] * 3,
        out_shape=[full, full, S(x.shape, BF16), S((1, WIDE), F32), columns, columns, columns, S(wo.shape, BF16),
                   line, line, S((CHIPS, *parts), BF16)],
        scratch_shapes=[
            *[VMEM(heads, BF16)] * 4, VMEM((*chunk, HEAD), BF16),
            VMEM((2, ROWS), F32), VMEM(chunk, F32), VMEM(chunk, F32),
            VMEM((2, HEAD + 8, CHUNK), F32), VMEM((2, HEAD, CHUNK), F32),
            VMEM(heads, F32), VMEM(heads, F32),
            VMEM((ROWS, 768), BF16), VMEM((256, WIDE), F32), VMEM((2, MINE, WIDE), BF16),
            VMEM(parts, BF16), VMEM(quarts, BF16), VMEM((PART, WIDE), F32),
            VMEM((16, WIDE), F32), VMEM((CORES, 1, WIDE), F32),
            passed, came, passed, came,
            DMA((2,)), DMA((CHIPS, 2)), DMA((4,)), DMA((CHIPS, 4)), DMA((CHIPS, 4)), DMA((3,)), DMA((2,)), DMA((4,)),
            DMA((CORES,)), DMA((CORES,)),
        ],
        compiler_params=pltpu.CompilerParams(collective_id=0, has_side_effects=True, vmem_limit_bytes=66 * 10**6),
    )(a, x, dy, gain[None], tables[0], tables[1], tables[2], tables[3], wq, wk, wv, wo)
    return outs[2:8]


def solution(mesh):
    def step(x, dy, gain, wq, wk, wv, wo):
        wide, gain = x.astype(F32), gain.astype(F32)
        scale = lax.rsqrt(jnp.mean(wide * wide, -1, keepdims=True) + 1e-6)
        return heads_work((wide * scale * gain).astype(BF16), x, dy, gain, wq, wk, wv, wo)

    tokens, columns = P(("dp", "tp"), None), P(None, "tp")
    return jax.shard_map(
        step,
        mesh=mesh,
        in_specs=(tokens, tokens, P(None), columns, columns, columns, P("tp", None)),
        out_specs=(tokens, P("dp", None), P("dp", "tp"), P("dp", "tp"), P("dp", "tp"), P(("dp", "tp"), None)),
        check_vma=False,
    )
```

```python
import jax
import jax.numpy as jnp
import numpy as np
from jax import lax
from jax.experimental import pallas as pl
from jax.experimental.pallas import tpu as pltpu
from jax.sharding import PartitionSpec as P

HEAD = 128
THETA = 10000
NEG = -1e30
HIDDEN = 2 * NEG
LOG2E = 1.4426950408889634
MESH = pl.DeviceIdType.MESH
F32, BF16 = jnp.float32, jnp.bfloat16

CHIPS = 4
MINE = 512
PART = 256
WIDE = 2048
CHUNK = 2 * MINE
ROWS = CHIPS * CHUNK
SCALE = HEAD**-0.5
E2 = SCALE * LOG2E
BK = 512
PAIR = range(2)
SENDS = range(2)
SENT = MINE // len(SENDS)
CORES = 2 * CHIPS
QUART = PART // 4
PIECES = PART // QUART

STEPS = (
    "F3F2F1F0A3B3T3U3A2B2T2U2A1B1T1U1B0W0W1W2W3W4W5T0U0",
    "R0A0F3F2F1A3B3F0A2L0B2B1B0T3U3W0W1W2W3T2W4W5U2T0U0T1U1",
    "A3L0R0F3B3A1F2B2F1A0B1F0B0W0W1W2W3W4W5T3U3T1T0U0T2U1U2",
    "F3B3A2F2B2T2U2F1A1B1T1F0A0B0T0U0W0W1W2W3W4W5U1T3U3",
)
OPS = "-ARLFBTUW"


def _ds(i, size):
    return pl.ds(i * size if isinstance(i, int) else pl.multiple_of(i * size, size), size)


def _program():
    longest = max(map(len, STEPS)) // 2
    words, used = [], set()
    for i in range(longest):
        word = 0
        for steps in reversed(STEPS):
            op, arg = steps[2 * i : 2 * i + 2] or "-0"
            again = op in "TU" and (steps, op) in used
            used.add((steps, op))
            word = word * 128 + 8 * OPS.index(op) + int(arg) + 4 * again
        words.append(word)
    return words


def _dot(a, b, ca, cb):
    return lax.dot_general(a, b, (((ca,), (cb,)), ((), ())), preferred_element_type=F32)


def _pick(i, values):
    out = jnp.int32(values[-1])
    for n in range(len(values) - 2, -1, -1):
        out = jnp.where(i == n, jnp.int32(values[n]), out)
    return out


def _kernel(x_ref, dy_ref, gain, cosf, sinf, cosc, sinc, wq_ref, wk_ref, wv_ref, wo_ref,
            xf, dyf, by_x, by_gain, dwq_ref, dwk_ref, dwv_ref, dwo_ref, rin, lin, sin,
            wq, wk, wv, wo, dwq, dwk, dwv, dwo,
            q_s, k_s, v_s, out_s, do_s, lse_s, del_s, top_s, mix_s, dq_s, dk_s, dv_s, g_s, acc, tile, st, so, fin, gsum, gall,
            xs, xr, ys, yr, ss, sr, rs, rr, lr, loc, tsem, fsem, gs, gr, wsem):
    me = lax.axis_index("tp")
    z, c = lax.div(me, 2), lax.rem(me, 2)
    sib = me + 1 - 2 * c

    def rows(d, p):
        return _ds(len(SENDS) * d + p, SENT)

    def push(own, full, sends, recvs, d, p, kind, target, first):
        src = (own.at[p] if own is st else own.at[_ds(p, SENT), :]) if first else full.at[rows(d, p), :]
        pltpu.make_async_remote_copy(src_ref=src, dst_ref=full.at[rows(d, p), :], send_sem=sends.at[kind, d, p],
                                     recv_sem=recvs.at[d, p], device_id={"tp": target}, device_id_type=MESH).start()

    def waiting(full, sends, recvs, d, p, kind):
        return pltpu.make_async_remote_copy(src_ref=full.at[rows(d, p), :], dst_ref=full.at[rows(d, p), :], send_sem=sends.at[kind, d, p],
                                            recv_sem=recvs.at[d, p], device_id={"tp": sib}, device_id_type=MESH)

    X, Y = (st, xf, xs, xr), (dy_ref, dyf, ys, yr)

    def own_right(t):
        for p in SENDS:
            push(*t, me, p, 0, me + 2, True)

    def own_left(t):
        for p in SENDS:
            push(*t, me, p, 1, me - 2, True)

    def own_side(t):
        for p in SENDS:
            push(*t, me, p, 2, sib, True)

    def arrive(t, n):
        d = 2 * n + c
        right = n < z
        more = jnp.where(right, z < CHIPS - 1, z > 0)
        ahead = me + jnp.where(right, 2, -2)
        for p in SENDS:
            waiting(*t[1:], d, p, 0).wait_recv()

            @pl.when(more)
            def _():
                push(*t, d, p, 0, ahead, False)

            push(*t, d, p, 2, sib, False)

    taken = ((wq_ref, wq), (wk_ref, wk), (wv_ref, wv), (wo_ref, wo))
    for p in PAIR:
        pltpu.make_async_copy(x_ref.at[_ds(p, PART), :], tile.at[0, _ds(p, PART), :], tsem.at[p]).start()
    for i, (src, dst) in enumerate(taken):
        pltpu.make_async_copy(src, dst, wsem.at[i]).start()
    barrier = pltpu.get_barrier_semaphore()

    def greet(o, _):
        pl.semaphore_signal(barrier, inc=1, device_id={"tp": lax.rem(me + o, CORES)}, device_id_type=MESH)

    lax.fori_loop(1, CORES, greet, None)
    for p in PAIR:
        pltpu.make_async_copy(x_ref.at[_ds(p, PART), :], tile.at[0, _ds(p, PART), :], tsem.at[p]).wait()

        def forth(r, _):
            wide = tile[0, _ds(p * (PART // 16) + r, 16), :].astype(F32)
            scale = lax.rsqrt(jnp.mean(wide * wide, -1, keepdims=True) + 1e-6)
            st[p, _ds(r, 16), :] = (wide * scale * gain[:].astype(F32)).astype(BF16)

        lax.fori_loop(0, PART // 16, forth, None)
    pl.semaphore_wait(barrier, CORES - 1)

    @pl.when(z < CHIPS - 1)
    def _():
        own_right(X)

    @pl.when(z > 0)
    def _():
        own_left(X)

    own_side(X)
    for p in PAIR:
        pltpu.make_async_copy(st.at[p], xf.at[rows(me, p), :], tsem.at[p]).start()

    @pl.when(z == 0)
    def _():
        own_right(Y)

    @pl.when(z == CHIPS - 1)
    def _():
        own_left(Y)

    own_side(Y)
    dk_s[:] = jnp.zeros_like(dk_s)
    dv_s[:] = jnp.zeros_like(dv_s)
    acc[:] = jnp.zeros_like(acc)
    gsum[:] = jnp.zeros_like(gsum)

    for p in PAIR:
        pltpu.make_async_copy(st.at[p], xf.at[rows(me, p), :], tsem.at[p]).wait()
    for i, (src, dst) in enumerate(taken):
        pltpu.make_async_copy(src, dst, wsem.at[i]).wait()

    def angles(row):
        b = pl.ds(lax.div(row, 256), 1)
        cc, sc = cosc[b, :], sinc[b, :]
        cos = cc * cosf[:] - sc * sinf[:]
        s = sc * cosf[:] + cc * sinf[:]
        lane = lax.broadcasted_iota(jnp.int32, (256, HEAD), 1)
        return cos, jnp.where(lane < HEAD // 2, -s, s)

    def block_of(t, d, slot):
        return pltpu.make_async_copy(t[1].at[_ds(d, MINE), :], tile.at[slot], tsem.at[slot])

    def fetch(t, d, slot):
        if t is X:
            block_of(t, d, slot).start()
        else:
            @pl.when(d == me)
            def _():
                pltpu.make_async_copy(t[0], tile.at[slot], tsem.at[slot]).start()

            @pl.when(d != me)
            def _():
                block_of(t, d, slot).start()

    def fetched(t, slot):
        block_of(t, me, slot).wait()

    def project(i, _):
        j, h = lax.div(i, 2), lax.rem(i, 2)
        n = jnp.where(j == 0, z, jnp.where(j == 1, _pick(z, [1, 0, 1, 2]), jnp.where(j == 2, _pick(z, [2, 2, 3, 1]), _pick(z, [3, 3, 0, 0]))))
        d = 2 * n + jnp.where(h == 0, c, 1 - c)

        @pl.when((h == 0) & (j > 0))
        def _():
            arrive(X, n)

        @pl.when(h == 1)
        def _():
            for p in SENDS:
                waiting(*X[1:], d, p, 0).wait_recv()

        fetch(X, d, 0)
        fetched(X, 0)

        def sub(t, _):
            row = pl.multiple_of(d * MINE + t * 256, 256)
            some = tile[0, _ds(t, 256), :]
            cos, sgn = angles(row)
            for w, to, turn in ((wq, q_s, True), (wk, k_s, True), (wv, v_s, False)):
                got = _dot(some, w[:], 1, 0).astype(BF16)
                for head in PAIR:
                    one = got[:, _ds(head, HEAD)]
                    if turn:
                        wide = one.astype(F32)
                        one = (wide * cos + pltpu.roll(wide, HEAD // 2, 1) * sgn).astype(BF16)
                    to[head, pl.ds(row, 256), :] = one

        lax.fori_loop(0, 2, sub, None)

    lax.fori_loop(0, CORES, project, None)

    for p in SENDS:
        for kind, sent in enumerate((z < CHIPS - 1, z > 0, z >= 0)):
            @pl.when(sent)
            def _():
                waiting(*X[1:], me, p, kind).wait_send()

    seen = lax.broadcasted_iota(jnp.int32, (BK, BK), 1) >= lax.broadcasted_iota(jnp.int32, (BK, BK), 0)
    ones = jnp.ones((8, BK), BF16)
    WHOLE = [(0, 0, False), (0, 1, False), (1, 0, False), (1, 1, False)]
    CUT = [(0, 0, True), (0, 1, False), (1, 0, True), (1, 1, False)]
    LAST = [(0, 1, True), (1, 1, True)]

    def strip(n, s):
        return _ds(2 * n + s, BK)

    def cols(s):
        return _ds(s, BK)

    def ahead(n):
        top_s[:] = jnp.full_like(top_s, NEG)
        mix_s[:] = jnp.zeros_like(mix_s)

        def block(j, pieces):
            here = _ds(j, BK)
            scores = [_dot(k_s[i, here, :], q_s[i, strip(n, s), :], 1, 1) for i, s, _ in pieces]
            weights, keeps = [], []
            for (i, s, masked), sc in zip(pieces, scores):
                if masked:
                    sc = jnp.where(seen, sc, HIDDEN)
                old = top_s[i : i + 1, cols(s)]
                top = jnp.maximum(old, sc.max(axis=0, keepdims=True))
                top_s[i : i + 1, cols(s)] = top
                weights.append(jnp.exp2((sc - top) * E2).astype(BF16))
                keeps.append(jnp.exp2((old - top) * E2))
            for (i, s, _), p, keep in zip(pieces, weights, keeps):
                values = jnp.concatenate([v_s[i, here, :].T, ones], axis=0)
                mix_s[i, :, cols(s)] = mix_s[i, :, cols(s)] * keep + _dot(values, p, 1, 0)

        lax.fori_loop(0, 2 * n, lambda j, _: block(j, WHOLE), None)
        block(2 * n, CUT)
        block(2 * n + 1, LAST)
        here = _ds(n, CHUNK)
        for i in PAIR:
            total = mix_s[i, HEAD : HEAD + 1, :]
            out_s[i, here, :] = (mix_s[i, :HEAD, :] * (1 / total)).T.astype(BF16)
            lse_s[i : i + 1, here] = top_s[i : i + 1, :] * E2 + jnp.log(total) * LOG2E

    def term(row, store):
        def sub(b, _):
            at = _ds(b, 512)
            total = None
            for m, w in enumerate((wq, wk, wv)):
                t = _dot(g_s[pl.ds(row, 256), m * 256 : (m + 1) * 256], w[at, :], 1, 1)
                total = t if total is None else total + t
            store(at, total)

        lax.fori_loop(0, WIDE // 512, sub, None)

    def side_copy(n, p):
        return pltpu.make_async_remote_copy(src_ref=st.at[p], dst_ref=sin.at[n, p], send_sem=ss.at[p], recv_sem=sr.at[n, p],
                                            device_id={"tp": sib}, device_id_type=MESH)

    def line_copy(n, s, right):
        recv, to, ahead = (rr, rin, me + 2) if right else (lr, lin, me - 2)
        return pltpu.make_async_remote_copy(src_ref=so.at[s], dst_ref=to.at[n, s], send_sem=rs.at[s], recv_sem=recv.at[n, s],
                                            device_id={"tp": ahead}, device_id_type=MESH)

    def back(n):
        for p in SENDS:
            waiting(*Y[1:], 2 * n + 1 - c, p, 0).wait_recv()
        for h in PAIR:
            fetch(Y, 2 * n + h, h)
        for h in PAIR:
            fetched(Y, h)

            def sub(t, _):
                some = tile[h, _ds(t, 256), :]
                got = _dot(some, wo[:], 1, 1).astype(BF16)
                at = _ds(2 * h + t, 256)
                for i in PAIR:
                    do_s[i, at, :] = got[:, _ds(i, HEAD)]

            lax.fori_loop(0, 2, sub, None)
        here = _ds(n, CHUNK)
        for i in PAIR:
            del_s[i : i + 1, :] = (do_s[i].astype(F32) * out_s[i, here, :].astype(F32)).T.sum(axis=0, keepdims=True)
        dq_s[:] = jnp.zeros_like(dq_s)

        def block(j, pieces):
            keys = _ds(j, BK)
            qs = [q_s[i, strip(n, s), :] for i, s, _ in pieces]
            dos = [do_s[i, cols(s), :] for i, s, _ in pieces]
            scores = [_dot(k_s[i, keys, :], x, 1, 1) for (i, _, _), x in zip(pieces, qs)]
            dps = [_dot(v_s[i, keys, :], x, 1, 1) for (i, _, _), x in zip(pieces, dos)]
            for m, (i, s, masked) in enumerate(pieces):
                p = jnp.exp2(scores[m] * E2 - lse_s[i : i + 1, strip(n, s)])
                if masked:
                    p = jnp.where(seen, p, 0.0)
                ds = (p * (dps[m] - del_s[i : i + 1, cols(s)])).astype(BF16)
                dv_s[i, keys, :] += _dot(p.astype(BF16), dos[m], 1, 0)
                dk_s[i, keys, :] += _dot(ds, qs[m], 1, 0)
                dq_s[i, :, cols(s)] += _dot(k_s[i, keys, :].T, ds, 1, 0)

        lax.fori_loop(0, 2 * n, lambda j, _: block(j, WHOLE), None)
        block(2 * n, CUT)
        block(2 * n + 1, LAST)

        for t in range(CHUNK // 256):
            row = pl.multiple_of(n * CHUNK + t * 256, 256)
            cos, sgn = angles(row)
            for i in PAIR:
                dq = (dq_s[i, :, t * 256 : (t + 1) * 256] * SCALE).T
                dk = dk_s[i, pl.ds(row, 256), :] * SCALE
                for m, one in ((0, dq), (1, dk)):
                    g_s[pl.ds(row, 256), m * 256 + i * HEAD : m * 256 + (i + 1) * HEAD] = (
                        one * cos - pltpu.roll(one, HEAD // 2, 1) * sgn).astype(BF16)
                g_s[pl.ds(row, 256), 512 + i * HEAD : 512 + (i + 1) * HEAD] = dv_s[i, pl.ds(row, 256), :].astype(BF16)

        for p in PAIR:
            @pl.when(n < CHIPS - 1)
            def _():
                side_copy(n, p).wait_send()

            def store(at, value):
                st[p, :, at] = value.astype(BF16)

            term(pl.multiple_of((2 * n + 1 - c) * MINE + p * PART, PART), store)
            side_copy(n, p).start()

        for h in PAIR:
            mixed = _ds(2 * n + h, MINE)
            for i in PAIR:
                turned = out_s[i, mixed, :].T

                def wide(b, _):
                    at = _ds(b, 512)
                    acc[_ds(i, HEAD), at] += _dot(turned, tile[h, :, at], 1, 0)

                lax.fori_loop(0, WIDE // 512, wide, None)

        @pl.when(n == 0)
        def _():
            dwo[:] = acc[:].astype(BF16)
            pltpu.make_async_copy(dwo, dwo_ref, wsem.at[3]).start()

    def relay(n, p, again):
        from_left = (z <= n) & (z > 0)
        from_right = (z >= n) & (z < CHIPS - 1)
        here = tile.at[0, _ds(0, PART), :], tile.at[0, _ds(PIECES, QUART), :], tile.at[0, _ds(PIECES + 1, QUART), :]
        mine = ((x_ref, tile.at[1, _ds(0, PART), :]), (dy_ref, tile.at[1, _ds(1, PART), :]))

        @pl.when(z == n)
        def _():
            for i, (src, dst) in enumerate(mine):
                pltpu.make_async_copy(src.at[_ds(p, PART), :], dst, tsem.at[i]).start()

        side_copy(n, p).wait_recv()
        pltpu.make_async_copy(sin.at[n, p], here[0], loc.at[0]).start()

        def store(at, value):
            fin[:, at] = value

        term(pl.multiple_of((2 * n + c) * MINE + p * PART, PART), store)
        pltpu.make_async_copy(sin.at[n, p], here[0], loc.at[0]).wait()
        fin[:] += here[0][:].astype(F32)

        @pl.when(z == n)
        def _():
            for i, (src, dst) in enumerate(mine):
                pltpu.make_async_copy(src.at[_ds(p, PART), :], dst, tsem.at[i]).wait()

        def quarter(h, _):
            s = PIECES * p + h
            part = _ds(h, QUART)
            for i, (come, arrived, right) in enumerate(((from_left, rin, True), (from_right, lin, False))):
                @pl.when(come)
                def _():
                    line_copy(n, s, right).wait_recv()
                    pltpu.make_async_copy(arrived.at[n, s], here[1 + i], loc.at[1 + i]).start()

            for i, (come, arrived, right) in enumerate(((from_left, rin, True), (from_right, lin, False))):
                @pl.when(come)
                def _():
                    pltpu.make_async_copy(arrived.at[n, s], here[1 + i], loc.at[1 + i]).wait()
                    fin[part, :] += here[1 + i][:].astype(F32)

            @pl.when(again)
            def _():
                line_copy(n, s, True).wait_send()

            @pl.when(z != n)
            def _():
                so[s] = fin[part, :].astype(BF16)

            @pl.when(z < n)
            def _():
                line_copy(n, s, True).start()

            @pl.when(z > n)
            def _():
                line_copy(n, s, False).start()

            @pl.when(z == n)
            def _():
                def norm(r, _):
                    da = fin[_ds(h * (QUART // 16) + r, 16), :]
                    wide = tile[1, _ds(h * (QUART // 16) + r, 16), :].astype(F32)
                    straight = tile[1, _ds((PIECES + h) * (QUART // 16) + r, 16), :].astype(F32)
                    scale = lax.rsqrt(jnp.mean(wide * wide, -1, keepdims=True) + 1e-6)
                    unit = wide * scale
                    gsum[:] += da * unit
                    t = da * gain[:].astype(F32)
                    so[s, _ds(r, 16), :] = (scale * (t - unit * jnp.mean(t * unit, -1, keepdims=True)) + straight).astype(BF16)

                lax.fori_loop(0, QUART // 16, norm, None)
                pltpu.make_async_copy(so.at[s], by_x.at[_ds(s, QUART), :], fsem.at[s]).start()

        lax.fori_loop(0, PIECES, quarter, None)

    def weight(m, h):
        first = h * CHIPS
        fetch(X, first, 0)

        @pl.when(h == 0)
        def _():
            acc[:] = jnp.zeros_like(acc)

        def step(i, _):
            slot = lax.rem(i, 2)

            @pl.when(i + 1 < CHIPS)
            def _():
                fetch(X, first + i + 1, 1 - slot)

            fetched(X, slot)
            turned = g_s[_ds(first + i, MINE), _ds(m, 256)].T

            def wide(b, _):
                at = _ds(b, 512)
                acc[:, at] += _dot(turned, tile[slot, :, at], 1, 0)

            lax.fori_loop(0, WIDE // 512, wide, None)

        lax.fori_loop(0, CHIPS, step, None)
        for i, (to, out) in enumerate(((dwq, dwq_ref), (dwk, dwk_ref), (dwv, dwv_ref))):
            @pl.when((h == 1) & (m == i))
            def _():
                def turn(b, _):
                    to[_ds(b, 256), :] = acc[:, _ds(b, 256)].T.astype(BF16)

                lax.fori_loop(0, WIDE // 256, turn, None)
                pltpu.make_async_copy(to, out, wsem.at[i]).start()

    def step(i, _):
        word = _pick(i, words)
        code = lax.rem(_pick(z, [lax.div(word, jnp.int32(128**n)) for n in range(CHIPS)]), 128)
        op, arg = lax.div(code, 8), lax.rem(code, 8)

        def on(letter, do):
            pl.when(op == OPS.index(letter))(do)

        on("A", lambda: arrive(Y, arg))
        on("R", lambda: own_right(Y))
        on("L", lambda: own_left(Y))
        on("F", lambda: ahead(arg))
        on("B", lambda: back(arg))

        @pl.when((op == OPS.index("T")) | (op == OPS.index("U")))
        def _():
            relay(lax.rem(arg, CHIPS), op - OPS.index("T"), arg >= CHIPS)

        on("W", lambda: weight(lax.div(arg, 2), lax.rem(arg, 2)))

    words = _program()
    lax.fori_loop(0, len(words), step, None)

    def sum_copy(o, d):
        return pltpu.make_async_remote_copy(src_ref=gall.at[d], dst_ref=gall.at[d], send_sem=gs.at[o], recv_sem=gr.at[d],
                                            device_id={"tp": lax.rem(me + o, CORES)}, device_id_type=MESH)

    gall[me] = gsum[:].sum(axis=0, keepdims=True)
    lax.fori_loop(1, CORES, lambda o, _: sum_copy(o, me).start(), None)
    lax.fori_loop(1, CORES, lambda o, _: sum_copy(o, lax.rem(me + o, CORES)).wait_recv(), None)
    total = gall[0]
    for d in range(1, CORES):
        total = total + gall[d]
    by_gain[:] = total
    lax.fori_loop(1, CORES, lambda o, _: sum_copy(o, me).wait_send(), None)

    for i, (to, out) in enumerate(((dwq, dwq_ref), (dwk, dwk_ref), (dwv, dwv_ref), (dwo, dwo_ref))):
        pltpu.make_async_copy(to, out, wsem.at[i]).wait()
    for s in range(MINE // QUART):
        pltpu.make_async_copy(so.at[s], by_x.at[_ds(s, QUART), :], fsem.at[s]).wait()
    for p in PAIR:
        side_copy(0, p).wait_send()
    for p in SENDS:
        @pl.when(z < CHIPS - 1)
        def _():
            waiting(*Y[1:], me, p, 0).wait_send()

        @pl.when(z > 0)
        def _():
            waiting(*Y[1:], me, p, 1).wait_send()

        waiting(*Y[1:], me, p, 2).wait_send()
        for t in (X, Y):
            for n in range(CHIPS):
                @pl.when(n != z)
                def _():
                    waiting(*t[1:], 2 * n + c, p, 2).wait_send()

                @pl.when(((n < z) & (z < CHIPS - 1)) | ((n > z) & (z > 0)))
                def _():
                    waiting(*t[1:], 2 * n + c, p, 0).wait_send()


def heads_work(x, dy, gain, wq, wk, wv, wo):
    half = HEAD // 2
    rate = np.tile(float(THETA) ** (-np.arange(half) / half), 2)
    fine, coarse = np.arange(PART)[:, None] * rate, np.arange(0, ROWS, PART)[:, None] * rate
    tables = [jnp.asarray(f(t), F32) for t in (fine, coarse) for f in (np.cos, np.sin)]
    any_, vmem = pl.BlockSpec(memory_space=pl.ANY), pl.BlockSpec(memory_space=pltpu.VMEM)
    S = jax.ShapeDtypeStruct
    DMA, VMEM = pltpu.SemaphoreType.DMA, pltpu.VMEM
    heads, chunk = (2, ROWS, HEAD), (2, CHUNK)
    parts, quarts = (MINE // PART, PART, WIDE), (MINE // QUART, QUART, WIDE)
    full, line = S((ROWS, WIDE), BF16), S((CHIPS, *quarts), BF16)
    columns, pieces = S(wq.shape, BF16), MINE // QUART
    passed, came = DMA((3, CORES, len(SENDS))), DMA((CORES, len(SENDS)))
    outs = pl.pallas_call(
        _kernel,
        in_specs=[any_] * 2 + [vmem] * 5 + [any_] * 4,
        out_specs=[any_] * 3 + [vmem] + [any_] * 7,
        out_shape=[full, full, S(x.shape, BF16), S((1, WIDE), F32), columns, columns, columns, S(wo.shape, BF16),
                   line, line, S((CHIPS, *parts), BF16)],
        scratch_shapes=[
            *[VMEM(w.shape, BF16) for w in (wq, wk, wv, wo)] * 2,
            *[VMEM(heads, BF16)] * 4, VMEM((*chunk, HEAD), BF16),
            VMEM((2, ROWS), F32), VMEM(chunk, F32), VMEM(chunk, F32),
            VMEM((2, HEAD + 8, CHUNK), F32), VMEM((2, HEAD, CHUNK), F32),
            VMEM(heads, F32), VMEM(heads, F32),
            VMEM((ROWS, 768), BF16), VMEM((256, WIDE), F32), VMEM((2, MINE, WIDE), BF16),
            VMEM(parts, BF16), VMEM(quarts, BF16), VMEM((PART, WIDE), F32),
            VMEM((16, WIDE), F32), VMEM((CORES, 1, WIDE), F32),
            passed, came, passed, came,
            DMA((2,)), DMA((CHIPS, 2)), DMA((pieces,)), DMA((CHIPS, pieces)), DMA((CHIPS, pieces)), DMA((3,)), DMA((2,)), DMA((pieces,)),
            DMA((CORES,)), DMA((CORES,)), DMA((CHIPS,)),
        ],
        compiler_params=pltpu.CompilerParams(collective_id=0, has_side_effects=True, vmem_limit_bytes=66 * 10**6),
    )(x, dy, gain[None], tables[0], tables[1], tables[2], tables[3], wq, wk, wv, wo)
    return outs[2:8]


def solution(mesh):
    def step(x, dy, gain, wq, wk, wv, wo):
        return heads_work(x, dy, gain, wq, wk, wv, wo)

    tokens, columns = P(("dp", "tp"), None), P(None, "tp")
    return jax.shard_map(
        step,
        mesh=mesh,
        in_specs=(tokens, tokens, P(None), columns, columns, columns, P("tp", None)),
        out_specs=(tokens, P("dp", None), P("dp", "tp"), P("dp", "tp"), P("dp", "tp"), P(("dp", "tp"), None)),
        check_vma=False,
    )
```
